256 devices in a mesh: bl: 32 (over z, x), tm: 8 (over y, core).
Axes of the slice: x: 4, y: 4, z: 8, core: 2. Of those that a mesh axis runs over, the one named last changes fastest.
Arguments:
- visibility_real: bfloat16 [12288, 32, 1024], P('bl', 'tm'), may hold values from -6 to 6
- visibility_imag: bfloat16 [12288, 32, 1024], P('bl', 'tm'), may hold values from -6 to 6
- weights: int32 [12288, 32], P('bl', 'tm'), may hold values from 0 to 8
- labels: int32 [12288], P('bl'), may hold values from 0 to 2047, as said below
- owner_of: int32 [2048], replicated, may hold values from 0 to 31, as said below
Outputs:
- bandpower: float32 [2048, 1024], P(('bl', 'tm'))
The draws below stay inside these ranges and needn't reach their ends.
Inputs may be any that keep to these rules, and one draw needn't show every extreme that they name: Of the rows of one device, at most 18 have labels of groups with one owner, and these carry at most 4 different labels; in every draw some owner gets exactly 18 such rows with exactly 4 labels from every device. `owner_of`: every owner owns exactly 64 groups.
All inputs are finite; a program needn't handle non-finite values.
Results may differ from the reference program's by a relative error of at most 0.0003.
Values may be sent and summed in bfloat16 or wider, within the bound.
A program may use at most 128 MiB of HBM per device.

```python
import math
import jax
import jax.numpy as jnp
from jax import lax

FREQ_CHANNELS = 1024
B_DEV = 384
G_DEV = 64
BASELINE_COUNT = 12288
TIME_STEPS = 32
CAP = 18
KEYS = 4
N_BL = 32


def layout_plan(key):
    groups = G_DEV * N_BL
    group_order = jax.random.permutation(jax.random.fold_in(key, 101), groups).astype(jnp.int32)
    owner_of = jnp.zeros((groups,), jnp.int32).at[group_order].set(jnp.arange(groups, dtype=jnp.int32) // G_DEV)
    heaviest_owner = jax.random.randint(jax.random.fold_in(key, 102), (), 0, N_BL)

    def one_device(device):
        device_key = jax.random.fold_in(jax.random.fold_in(key, 103), device)
        slot_ids = jnp.arange(N_BL * CAP, dtype=jnp.int32)
        priority = jax.random.permutation(jax.random.fold_in(device_key, 1), N_BL * CAP).astype(jnp.int32)
        priority = jnp.where(slot_ids // CAP == heaviest_owner, priority - N_BL * CAP, priority)
        chosen = jnp.argsort(priority)[:B_DEV].astype(jnp.int32)
        target = chosen // CAP
        within = chosen % CAP

        def candidates(owner):
            owner_key = jax.random.fold_in(jax.random.fold_in(device_key, 2), owner)
            return jax.random.permutation(owner_key, G_DEV)[:KEYS].astype(jnp.int32)
        offsets = jax.vmap(candidates)(jnp.arange(N_BL, dtype=jnp.int32))
        picked = offsets[target, within % KEYS]
        row_label = group_order[target * G_DEV + picked]
        shuffle = jax.random.permutation(jax.random.fold_in(device_key, 3), B_DEV)
        return row_label[shuffle]
    labels = jax.vmap(one_device)(jnp.arange(N_BL, dtype=jnp.int32)).reshape(-1)
    return (labels.astype(jnp.int32), owner_of)


def draw_labels(key, part):
    return layout_plan(key)[0]


def draw_owner_of(key, part):
    return layout_plan(key)[1]


def set_ends(values, stream_key, low, top_value):
    dims = values.shape
    index_at = [jax.random.randint(jax.random.fold_in(stream_key, axis), (), 0, dims[axis]) for axis in range(len(dims))]
    values = values.at[tuple(index_at)].set(low)
    longest = dims.index(max(dims))
    index_at[longest] = (index_at[longest] + 1) % dims[longest]
    return values.at[tuple(index_at)].set(top_value)


def shard_levels(key, dims, split, smallest, largest):
    loudness = 1.0
    for dim, blocks in split:
        draws = jax.random.uniform(jax.random.fold_in(jax.random.fold_in(key, 6), dim), (blocks,), jnp.float32, smallest / len(split), largest / len(split))
        loudness = loudness * jnp.repeat(jnp.exp(draws), dims[dim] // blocks).reshape((-1,) + (1,) * (len(dims) - 1 - dim))
    return loudness


def noise(key, shape, width, reach, shards=(), kind=jnp.bfloat16):
    level = shard_levels(key, shape, shards, -0.22, 0.18) if shards else 1.0
    array = jax.random.normal(key, shape, jnp.float32) * width * level
    return jnp.minimum(jnp.maximum(array, -reach), reach).astype(kind)


def setup_inputs(seed: int = 0) -> dict:
    keys = jax.random.split(jax.random.key(seed), 6)
    return {
        "visibility_real": noise(keys[0], (BASELINE_COUNT, TIME_STEPS, FREQ_CHANNELS), 1.0, 6.0, ((0, 32), (1, 8))),
        "visibility_imag": noise(keys[1], (BASELINE_COUNT, TIME_STEPS, FREQ_CHANNELS), 1.0, 6.0, ((0, 32), (1, 8))),
        "weights": set_ends(jax.random.randint(keys[2], (BASELINE_COUNT, TIME_STEPS), 0, 9), jax.random.fold_in(keys[2], 1), 0, 8).astype(jnp.int32),
        "labels": draw_labels(jax.random.fold_in(keys[5], 71), 0),
        "owner_of": draw_owner_of(jax.random.fold_in(keys[5], 71), 0),
    }


HARRIS = (0.35875, 0.48829, 0.14128, 0.01168)

def taper_of(length):
    phase_angle = 2.0 * math.pi / length * jnp.arange(length, dtype=jnp.float32)
    return HARRIS[0] - HARRIS[1] * jnp.cos(phase_angle) + HARRIS[2] * jnp.cos(2.0 * phase_angle) - HARRIS[3] * jnp.cos(3.0 * phase_angle)

def reference(visibility_real, visibility_imag, weights, labels, owner_of):
    groups = owner_of.shape[0]
    channels = visibility_real.shape[2]
    times = visibility_real.shape[1]
    window_taper = taper_of(channels)
    window_taper = window_taper / jnp.sqrt(jnp.sum(window_taper * window_taper))

    def advance(carried, instant):
        prior_real, prior_imag, running = carried
        row_weight = lax.dynamic_index_in_dim(weights, instant, 1, keepdims=False).astype(jnp.float32)
        slab_real = lax.dynamic_index_in_dim(visibility_real, instant, 1, keepdims=False).astype(jnp.float32)
        slab_imag = lax.dynamic_index_in_dim(visibility_imag, instant, 1, keepdims=False).astype(jnp.float32)
        sum_real = jax.ops.segment_sum(row_weight[:, None] * slab_real, labels, num_segments=groups)
        sum_imag = jax.ops.segment_sum(row_weight[:, None] * slab_imag, labels, num_segments=groups)
        weight_sum = jax.ops.segment_sum(row_weight, labels, num_segments=groups)
        divisor = jnp.maximum(weight_sum, 1.0)[:, None]
        mean_real = sum_real / divisor
        mean_imag = sum_imag / divisor
        spectrum = jnp.fft.fft((mean_real + 1j * mean_imag) * window_taper[None, :], axis=1)
        spec_real = jnp.real(spectrum)
        spec_imag = jnp.imag(spectrum)
        cross = prior_real * spec_real + prior_imag * spec_imag
        running = running + jnp.where(instant > 0, cross, jnp.zeros_like(cross))
        return ((spec_real, spec_imag, running), instant)
    zeros = jnp.zeros((groups, channels), jnp.float32)
    final_state, unused = lax.scan(advance, (zeros, zeros, zeros), jnp.arange(times, dtype=jnp.int32))
    order = jnp.argsort(owner_of * groups + jnp.arange(groups, dtype=jnp.int32))
    return final_state[2][order]
```

```python
import functools
import math

import jax
import jax.numpy as jnp
import numpy as np
from jax import lax
from jax.experimental import pallas as pl
from jax.experimental.pallas import tpu as pltpu
from jax.sharding import PartitionSpec as P

HARRIS = (0.35875, 0.48829, 0.14128, 0.01168)
MESH = pl.DeviceIdType.MESH
F32, BF16, I32 = jnp.float32, jnp.bfloat16, jnp.int32

OFFSETS = [
    (dz, dx) for dx in (0, 1, 2, 3) for dz in (1, 7, 2, 6, 3, 5, 4, 0) if (dz, dx) != (0, 0)
]


def taper_row(length):
    angle = 2.0 * np.pi / length * np.arange(length)
    h = (
        HARRIS[0]
        - HARRIS[1] * np.cos(angle)
        + HARRIS[2] * np.cos(2.0 * angle)
        - HARRIS[3] * np.cos(3.0 * angle)
    )
    return (h / np.sqrt(np.sum(h * h)))[None, :].astype(np.float32)


def dft_constants(length):
    n = length // 4
    angle = 2.0 * np.pi / n * (np.outer(np.arange(n), np.arange(n)) % n)
    c, s = np.cos(angle), np.sin(angle)
    table = np.block([[c, -s], [s, c]]).astype(np.float32)
    high = table.astype(jnp.bfloat16)
    low = (table - high.astype(np.float32)).astype(jnp.bfloat16)
    turn = 2.0 * np.pi / length * np.outer(np.arange(4), np.arange(n))
    twiddle = np.concatenate([np.cos(turn), np.sin(turn)], axis=0).astype(np.float32)
    return high, low, twiddle


def iota(shape, dim):
    return lax.broadcasted_iota(I32, shape, dim)


def dot(a, b):
    return jnp.dot(a, b, preferred_element_type=F32)


def dot_t(a, b):
    return lax.dot_general(a, b, (((1,), (1,)), ((), ())), preferred_element_type=F32)


def index_rows(labels_ref, owner_ref, sel):
    rows = labels_ref.shape[1]
    blocks = owner_ref.shape[1] // 128
    columns = []
    for b in range(rows // 128):
        piece = labels_ref[:, 128 * b : 128 * b + 128].astype(F32)
        columns.append(jnp.transpose(jnp.broadcast_to(piece, (128, 128))))
    label_col = jnp.concatenate(columns, axis=0)
    lane = iota((rows, 128), 1).astype(F32)
    owner_iota = iota((32, 128), 0)
    hits, marks = [], []
    for b in range(blocks):
        chosen = (label_col == lane + 128.0 * b).astype(F32)
        sel[:, 128 * b : 128 * b + 128] = chosen.astype(BF16)
        present = jnp.max(chosen, axis=0, keepdims=True)
        hit = (owner_ref[:, 128 * b : 128 * b + 128] == owner_iota).astype(F32)
        hits.append(hit)
        marks.append(hit)
        marks.append(hit * present)
    stacked = jnp.concatenate(marks, axis=0).astype(BF16)
    earlier = jnp.logical_or(iota((128, 256), 0) < iota((128, 256), 1), iota((128, 256), 1) >= 128)
    sums = dot(stacked, earlier.astype(F32).astype(BF16))
    before = jnp.zeros((64, 128), F32)
    row8 = iota((8, 128), 0)
    tables = []
    for b in range(blocks):
        within = sums[64 * b : 64 * b + 64]
        prefix = within[:, :128] + before
        before = before + within[:, 128:]
        rank = jnp.sum(hits[b] * prefix[:32], axis=0, keepdims=True)
        slot = jnp.sum(hits[b] * (prefix[32:] + 4.0 * owner_iota.astype(F32)), axis=0, keepdims=True)
        tables.append(jnp.where(row8 == 0, slot, jnp.where(row8 == 1, rank, 0.0)))
    table = jnp.concatenate(tables, axis=1).astype(BF16)
    return dot_t(table, sel[...])


def kernel(
    labels_ref, owner_ref, weights_ref, taper_ref, twiddle_ref, vis_re, vis_im, high_hbm, low_hbm,
    out_ref,
    raw, flat, sel, sent, held, meta_out, meta_in, table, first, after, parts, fb,
    load_sem, send_sem, recv_sem, meta_send, meta_recv, edge_send, edge_recv, part_send, part_recv,
):
    bl, tm = lax.axis_index("bl"), lax.axis_index("tm")
    z, x = bl // 4, bl % 4
    times, channels = 4, 1024
    rows = labels_ref.shape[1]

    loads = [
        pltpu.make_async_copy(vis_re, raw.at[0], load_sem.at[0]),
        pltpu.make_async_copy(vis_im, raw.at[1], load_sem.at[1]),
        pltpu.make_async_copy(high_hbm, table.at[0], load_sem.at[2]),
        pltpu.make_async_copy(low_hbm, table.at[1], load_sem.at[3]),
    ]
    for load in loads:
        load.start()

    def partner(offset):
        return ((z + offset[0]) % 8) * 4 + (x + offset[1]) % 4

    barrier = pltpu.get_barrier_semaphore()
    for offset in OFFSETS:
        pl.semaphore_signal(barrier, inc=1, device_id=(partner(offset), tm), device_id_type=MESH)
    for e in range(1, 8):
        pl.semaphore_signal(barrier, inc=1, device_id=(bl, (tm + e) % 8), device_id_type=MESH)

    found = index_rows(labels_ref, owner_ref, sel)
    spread = (iota((rows, 4 * rows), 1) // 4 == iota((rows, 4 * rows), 0)).astype(F32).astype(BF16)
    packed = jnp.concatenate(
        [found[0:1], weights_ref[...].astype(F32), jnp.zeros((3, rows), F32)], axis=0
    )
    wide = dot(packed.astype(BF16), spread)
    time_of = iota((1, 4 * rows), 1) % 4
    slot_wide = wide[0:1]
    weight_wide = jnp.zeros((1, 4 * rows), F32)
    for t in range(times):
        weight_wide = jnp.where(time_of == t, wide[1 + t : 2 + t], weight_wide)

    slot_iota = iota((128, 1), 0)
    slot_f = slot_iota.astype(F32)
    swapped_f = (slot_iota + 4 - 8 * ((slot_iota % 8) // 4)).astype(F32)
    lane = iota((128, 128), 1)
    row = iota((128, 128), 0)
    rank_col = jnp.max(jnp.where(found[0:1] == slot_f, found[1:2], 0.0), axis=1, keepdims=True)
    by_slot = jnp.where(lane == (row % 4) * 32, rank_col, 0.0)
    scale_even = jnp.zeros((128, 128), F32)
    scale_odd = jnp.zeros((128, 128), F32)

    loads[0].wait()
    loads[1].wait()
    for part in range(2):
        for j in range(4):
            flat[:, part * channels + 256 * j : part * channels + 256 * j + 256] = raw[
                part, :, :, 256 * j : 256 * j + 256
            ].reshape(4 * rows, 256)

    def send_chunk(t):
        for i, offset in enumerate(OFFSETS):
            to = partner(offset)
            pltpu.make_async_remote_copy(
                src_ref=sent.at[t, to % 2, to // 2],
                dst_ref=held.at[t, i + 1],
                send_sem=send_sem.at[t],
                recv_sem=recv_sem.at[t],
                device_id=(to, tm),
                device_id_type=MESH,
            ).start()

    top = (iota((128, 1), 0) % 8) < 4
    for t in range(times):
        slot_t = jnp.where(time_of == t, slot_wide, -1.0)
        fold_re = jnp.where(slot_t == slot_f, weight_wide, 0.0)
        fold_im = jnp.where(slot_t == swapped_f, weight_wide, 0.0)
        weight_col = jnp.sum(fold_re, axis=1, keepdims=True)
        by_slot = jnp.where(lane == (row % 4) * 32 + 1 + t, weight_col, by_slot)
        re = dot(fold_re.astype(BF16), flat[:, :channels])
        im = dot(fold_im.astype(BF16), flat[:, channels:])
        scales = []
        for parity in range(2):
            piece = jnp.where(top, re, im) if parity == 0 else jnp.where(top, im, re)
            largest = jnp.max(jnp.abs(piece), axis=1, keepdims=True)
            scale = jnp.maximum(largest, 1e-30) * (1.0079 / 32767.0)
            scale = scale.astype(BF16).astype(F32)
            scales.append(scale)
            code = jnp.round(piece * (1.0 / scale)).astype(I32)
            both = jnp.bitwise_or(
                jnp.left_shift(code[:, 512:], 16), jnp.bitwise_and(code[:, :512], 0xFFFF)
            )
            sent[t, parity] = both.reshape(16, 8, 512)
        here = lane == (row % 4) * 32 + 5 + 4 * ((row % 8) // 4) + t
        scale_even = jnp.where(here, scales[0], scale_even)
        scale_odd = jnp.where(here, scales[1], scale_odd)
        if t == times - 1:
            owner32, row32 = iota((32, 128), 0), iota((32, 128), 1)
            meta = (
                dot((row32 // 4 == owner32).astype(F32).astype(BF16), by_slot.astype(BF16))
                + dot((2 * (row32 // 8) == owner32).astype(F32).astype(BF16), scale_even.astype(BF16))
                + dot((2 * (row32 // 8) + 1 == owner32).astype(F32).astype(BF16), scale_odd.astype(BF16))
            )
            for o in range(32):
                meta_out[o] = meta[o : o + 1]
        if t == 0:
            pl.semaphore_wait(barrier, 38)
        if t == times - 1:
            for i, offset in enumerate(OFFSETS):
                to = partner(offset)
                pltpu.make_async_remote_copy(
                    src_ref=meta_out.at[to],
                    dst_ref=meta_in.at[i + 1],
                    send_sem=meta_send,
                    recv_sem=meta_recv,
                    device_id=(to, tm),
                    device_id_type=MESH,
                ).start()
        send_chunk(t)
        held[t, 0] = sent[t, bl % 2, bl // 2]
    meta_in[0] = meta_out[bl]

    loads[2].wait()
    loads[3].wait()
    pltpu.make_async_copy(meta_in.at[pl.ds(1, 31)], meta_in.at[pl.ds(1, 31)], meta_recv).wait()
    meta = jnp.concatenate([meta_in[i] for i in range(32)], axis=0)
    held_row, held_lane = iota((256, 128), 0), iota((256, 128), 1)
    expand = (iota((256, 32), 0) // 8 == iota((256, 32), 1)).astype(F32).astype(BF16)
    info = dot(expand, meta.astype(BF16))
    base = (held_row % 4) * 32
    flip = bl % 2

    def column(k):
        return jnp.sum(jnp.where(held_lane == base + k, info, 0.0), axis=1, keepdims=True)

    quadrant = jnp.where(flip == 0, (held_row % 8) // 4, 1 - (held_row % 8) // 4)
    chooser = jnp.where(
        jnp.logical_and(
            column(0) == (held_lane % 64).astype(F32), quadrant == held_lane // 64
        ),
        1.0,
        0.0,
    )
    chooser = jnp.transpose(chooser).astype(BF16)
    scale_cols, weight_mat = [], jnp.zeros((256, 128), F32)
    for t in range(times):
        scale_cols.append(column(5 + 4 * ((held_row % 8) // 4) + t))
        weight_mat = jnp.where(held_lane == t, column(1 + t), weight_mat)
    weight_sum = dot(chooser, weight_mat.astype(BF16))
    inverse = 1.0 / jnp.maximum(weight_sum, 1.0)

    cosine = [twiddle_ref[k : k + 1] for k in range(4)]
    sine = [twiddle_ref[4 + k : 5 + k] for k in range(4)]

    def spectrum(t):
        both = held[t].reshape(256, 512)
        low_part = jnp.right_shift(jnp.left_shift(both, 16), 16)
        high_part = jnp.right_shift(both, 16)
        arrived = jnp.concatenate([low_part, high_part], axis=1).astype(F32) * scale_cols[t]
        coarse = arrived.astype(BF16)
        fine = (arrived - coarse.astype(F32)).astype(BF16)
        total = dot(chooser, coarse) + dot(chooser, fine)
        mean = total * (inverse[:, t : t + 1] * taper_ref[...])
        xr = [mean[:64, 256 * j : 256 * j + 256] for j in range(4)]
        xi = [mean[64:, 256 * j : 256 * j + 256] for j in range(4)]
        ar, ai, cr, ci = xr[0] + xr[2], xi[0] + xi[2], xr[0] - xr[2], xi[0] - xi[2]
        br, bi, dr, di = xr[1] + xr[3], xi[1] + xi[3], xr[1] - xr[3], xi[1] - xi[3]
        yr = [ar + br, cr + di, ar - br, cr - di]
        yi = [ai + bi, ci - dr, ai - bi, ci + dr]
        stacked = []
        for k in range(4):
            re, im = yr[k], yi[k]
            if k:
                re, im = re * cosine[k] + im * sine[k], im * cosine[k] - re * sine[k]
            stacked.append(jnp.concatenate([re, im], axis=1))
        y = jnp.concatenate(stacked, axis=0)
        y_high = y.astype(BF16)
        y_low = (y - y_high.astype(F32)).astype(BF16)
        return dot(y_high, table[0]) + dot(y_low, table[0]) + dot(y_high, table[1])

    edge = pltpu.make_async_remote_copy(
        src_ref=first,
        dst_ref=after,
        send_sem=edge_send,
        recv_sem=edge_recv,
        device_id=(bl, (tm + 7) % 8),
        device_id_type=MESH,
    )
    power = None
    previous = None
    for t in range(times):
        pltpu.make_async_copy(
            held.at[t, pl.ds(1, 31)], held.at[t, pl.ds(1, 31)], recv_sem.at[t]
        ).wait()
        now = spectrum(t)
        if t == 0:
            first[...] = now
            edge.start()
        elif t == 1:
            power = previous * now
        else:
            power = power + previous * now
        previous = now
    edge.wait()
    power = power + jnp.where(tm < 7, previous * after[...], 0.0)
    power = power[:, :256] + power[:, 256:]
    for m in range(8):
        for k in range(4):
            parts[m, k] = power[64 * k + 8 * m : 64 * k + 8 * m + 8]
    for e in range(1, 8):
        to = (tm + e) % 8
        pltpu.make_async_remote_copy(
            src_ref=parts.at[to],
            dst_ref=fb.at[e],
            send_sem=part_send,
            recv_sem=part_recv,
            device_id=(bl, to),
            device_id_type=MESH,
        ).start()
    fb[0] = parts[tm]

    for t in range(times):
        pltpu.make_async_copy(
            held.at[t, pl.ds(1, 31)], held.at[t, pl.ds(1, 31)], send_sem.at[t]
        ).wait()
    pltpu.make_async_copy(meta_in.at[pl.ds(1, 31)], meta_in.at[pl.ds(1, 31)], meta_send).wait()
    pltpu.make_async_copy(fb.at[pl.ds(1, 7)], fb.at[pl.ds(1, 7)], part_send).wait()
    pltpu.make_async_copy(fb.at[pl.ds(1, 7)], fb.at[pl.ds(1, 7)], part_recv).wait()
    summed = fb[0]
    for e in range(1, 8):
        summed = summed + fb[e]
    out_ref[...] = summed


def interleave(x_ref, o_ref):
    lane = iota((8, 128), 1)
    for b in range(8):
        value = jnp.zeros((8, 128), F32)
        for k in range(4):
            source = x_ref[k, :, 128 * (b // 4) : 128 * (b // 4) + 128]
            taken = jnp.take_along_axis(source, 32 * (b % 4) + lane // 4, axis=1)
            value = jnp.where(lane % 4 == k, taken, value)
        o_ref[:, 128 * b : 128 * b + 128] = value


def per_device(visibility_real, visibility_imag, weights, labels, owner_of):
    rows, times, channels = visibility_real.shape
    high, low, twiddle = dft_constants(channels)
    taper = taper_row(channels)
    vmem = pl.BlockSpec(memory_space=pltpu.VMEM)
    hbm = pl.BlockSpec(memory_space=pl.ANY)
    dma = pltpu.SemaphoreType.DMA
    summed = pl.pallas_call(
        kernel,
        out_shape=jax.ShapeDtypeStruct((4, 8, 256), F32),
        in_specs=[vmem] * 5 + [hbm] * 4,
        out_specs=vmem,
        scratch_shapes=[
            pltpu.VMEM((2, rows, times, channels), BF16),
            pltpu.VMEM((rows * times, 2 * channels), BF16),
            pltpu.VMEM((rows, owner_of.shape[0]), BF16),
            pltpu.VMEM((times, 2, 16, 8, 512), I32),
            pltpu.VMEM((times, 32, 8, 512), I32),
            pltpu.VMEM((32, 1, 128), F32),
            pltpu.VMEM((32, 1, 128), F32),
            pltpu.VMEM((2, 512, 512), BF16),
            pltpu.VMEM((256, 512), F32),
            pltpu.VMEM((256, 512), F32),
            pltpu.VMEM((8, 4, 8, 256), F32),
            pltpu.VMEM((8, 4, 8, 256), F32),
            dma((4,)),
            dma((4,)),
            dma((4,)),
            dma(()),
            dma(()),
            dma(()),
            dma(()),
            dma(()),
            dma(()),
        ],
        compiler_params=pltpu.CompilerParams(
            collective_id=0, has_side_effects=True, vmem_limit_bytes=60 * 1024 * 1024
        ),
        name="bandpower",
    )(
        labels.reshape(1, rows), owner_of.reshape(1, -1), weights.T, jnp.asarray(taper),
        jnp.asarray(twiddle), visibility_real, visibility_imag, jnp.asarray(high), jnp.asarray(low),
    )
    return pl.pallas_call(
        interleave,
        out_shape=jax.ShapeDtypeStruct((8, channels), F32),
        in_specs=[vmem],
        out_specs=vmem,
        name="interleave",
    )(summed)


def solution(mesh):
    placed = (P("bl", "tm", None), P("bl", "tm", None), P("bl", "tm"), P("bl"), P())
    return jax.shard_map(
        per_device, mesh=mesh, in_specs=placed, out_specs=P(("bl", "tm"), None), check_vma=False
    )
```

```python
import functools
import math

import jax
import jax.numpy as jnp
import numpy as np
from jax import lax
from jax.experimental import pallas as pl
from jax.experimental.pallas import tpu as pltpu
from jax.sharding import PartitionSpec as P

HARRIS = (0.35875, 0.48829, 0.14128, 0.01168)
MESH = pl.DeviceIdType.MESH
F32, BF16, I32 = jnp.float32, jnp.bfloat16, jnp.int32

OFFSETS = [
    (dz, dx) for dx in (0, 1, 2, 3) for dz in (1, 7, 2, 6, 3, 5, 4, 0) if (dz, dx) != (0, 0)
]


def taper_row(length):
    angle = 2.0 * np.pi / length * np.arange(length)
    h = (
        HARRIS[0]
        - HARRIS[1] * np.cos(angle)
        + HARRIS[2] * np.cos(2.0 * angle)
        - HARRIS[3] * np.cos(3.0 * angle)
    )
    return (h / np.sqrt(np.sum(h * h)))[None, :].astype(np.float32)


def dft_constants(length):
    n = length // 4
    angle = 2.0 * np.pi / n * (np.outer(np.arange(n), np.arange(n)) % n)
    c, s = np.cos(angle), np.sin(angle)
    table = np.block([[c, -s], [s, c]]).astype(np.float32)
    high = table.astype(jnp.bfloat16)
    low = (table - high.astype(np.float32)).astype(jnp.bfloat16)
    turn = 2.0 * np.pi / length * np.outer(np.arange(4), np.arange(n))
    twiddle = np.concatenate([np.cos(turn), np.sin(turn)], axis=0).astype(np.float32)
    return high, low, twiddle


def iota(shape, dim):
    return lax.broadcasted_iota(I32, shape, dim)


def dot(a, b):
    return jnp.dot(a, b, preferred_element_type=F32)


def dot_t(a, b):
    return lax.dot_general(a, b, (((1,), (1,)), ((), ())), preferred_element_type=F32)


def index_rows(labels_ref, owner_ref):
    rows = labels_ref.shape[0]
    blocks = owner_ref.shape[0]
    labels = labels_ref[...].reshape(1, rows)
    high = (labels // 128 == iota((blocks, rows), 0)).astype(F32)
    low = (labels % 128 == iota((128, rows), 0)).astype(F32).astype(BF16)
    present = dot_t(high.astype(BF16), low)
    present = jnp.where(present > 0.0, 1.0, 0.0)
    owner_iota = iota((32, 128), 0)
    hits, marks = [], []
    for b in range(blocks):
        hit = (owner_ref[b : b + 1, :] == owner_iota).astype(F32)
        hits.append(hit)
        marks.append(hit)
        marks.append(hit * present[b : b + 1])
    stacked = jnp.concatenate(marks, axis=0).astype(BF16)
    earlier = jnp.logical_or(iota((128, 256), 0) < iota((128, 256), 1), iota((128, 256), 1) >= 128)
    sums = dot(stacked, earlier.astype(F32).astype(BF16))
    before = jnp.zeros((64, 128), F32)
    ranks, slots = [], []
    for b in range(blocks):
        within = sums[64 * b : 64 * b + 64]
        prefix = within[:, :128] + before
        before = before + within[:, 128:]
        ranks.append(jnp.sum(hits[b] * prefix[:32], axis=0, keepdims=True))
        first_slot = 4.0 * owner_iota.astype(F32)
        slots.append(jnp.sum(hits[b] * (prefix[32:] + first_slot), axis=0, keepdims=True))
    table = jnp.concatenate(slots + ranks, axis=0).astype(BF16)
    found = dot(table, low)
    slot = jnp.sum(high * found[:blocks], axis=0, keepdims=True)
    rank = jnp.sum(high * found[blocks:], axis=0, keepdims=True)
    return slot, rank


def kernel(
    labels_hbm, owner_hbm, weights_hbm, taper_hbm, twiddle_hbm, vis_re, vis_im, high_hbm, low_hbm,
    out_ref,
    labels_ref, owner_ref, weights_ref, taper_ref, twiddle_ref, raw, sums, sent, held,
    meta_out, meta_in, table, first, after, parts, fb,
    load_sem, send_sem, recv_sem, meta_send, meta_recv, edge_send, edge_recv, part_send, part_recv,
):
    bl, tm = lax.axis_index("bl"), lax.axis_index("tm")
    z, x = bl // 4, bl % 4
    times, channels = 4, 1024
    rows = labels_ref.shape[0]

    pairs = [
        (labels_hbm, labels_ref),
        (owner_hbm, owner_ref),
        (weights_hbm, weights_ref),
        (taper_hbm, taper_ref),
        (twiddle_hbm, twiddle_ref),
        (vis_re, raw.at[0]),
        (vis_im, raw.at[1]),
        (high_hbm, table.at[0]),
        (low_hbm, table.at[1]),
    ]
    loads = [
        pltpu.make_async_copy(source, target, load_sem.at[n])
        for n, (source, target) in enumerate(pairs)
    ]
    for load in loads:
        load.start()

    def partner(offset):
        return ((z + offset[0]) % 8) * 4 + (x + offset[1]) % 4

    barrier = pltpu.get_barrier_semaphore()
    for offset in OFFSETS:
        pl.semaphore_signal(barrier, inc=1, device_id=(partner(offset), tm), device_id_type=MESH)
    for e in range(1, 8):
        pl.semaphore_signal(barrier, inc=1, device_id=(bl, (tm + e) % 8), device_id_type=MESH)

    for n in range(5):
        loads[n].wait()
    slot_row, rank_row = index_rows(labels_ref, owner_ref)
    spread = (iota((rows, 4 * rows), 1) // 4 == iota((rows, 4 * rows), 0)).astype(F32).astype(BF16)
    packed = jnp.concatenate(
        [slot_row, weights_ref[...].astype(F32), jnp.zeros((3, rows), F32)], axis=0
    )
    wide = dot(packed.astype(BF16), spread)
    time_of = iota((1, 4 * rows), 1) % 4
    slot_wide = wide[0:1]
    weight_wide = jnp.zeros((1, 4 * rows), F32)
    for t in range(times):
        weight_wide = jnp.where(time_of == t, wide[1 + t : 2 + t], weight_wide)

    slot_f = iota((128, 1), 0).astype(F32)
    lane = iota((128, 256), 1)
    row = iota((128, 256), 0)
    by_slot = None
    scale_even = jnp.zeros((128, 256), F32)
    scale_odd = jnp.zeros((128, 256), F32)

    cosine = [twiddle_ref[k : k + 1] for k in range(4)]
    sine = [twiddle_ref[4 + k : 5 + k] for k in range(4)]
    top = (iota((128, 1), 0) % 8) < 4

    def send_chunk(h, t):
        for i, offset in enumerate(OFFSETS):
            to = partner(offset)
            pltpu.make_async_remote_copy(
                src_ref=sent.at[h, t, to % 2, to // 2],
                dst_ref=held.at[h, t, i + 1],
                send_sem=send_sem.at[h, t],
                recv_sem=recv_sem.at[h, t],
                device_id=(to, tm),
                device_id_type=MESH,
            ).start()

    def spectra(q, xr, xi):
        if q % 2 == 0:
            ar, ai, br, bi = xr[0] + xr[2], xi[0] + xi[2], xr[1] + xr[3], xi[1] + xi[3]
        else:
            ar, ai, br, bi = xr[0] - xr[2], xi[0] - xi[2], xi[1] - xi[3], xr[3] - xr[1]
        re, im = (ar + br, ai + bi) if q < 2 else (ar - br, ai - bi)
        if q:
            re, im = re * cosine[q] + im * sine[q], im * cosine[q] - re * sine[q]
        y = jnp.concatenate([re, im], axis=1)
        y_high = y.astype(BF16)
        y_low = (y - y_high.astype(F32)).astype(BF16)
        out = dot(y_high, table[0]) + dot(y_low, table[0]) + dot(y_high, table[1])
        return out[:, :256], out[:, 256:]

    folds = [
        jnp.where(jnp.where(time_of == t, slot_wide, -1.0) == slot_f, weight_wide, 0.0)
        for t in range(times)
    ]

    def fold_sums(fold):
        fold = fold.astype(BF16)
        both = []
        for part in range(2):
            if fold.shape[0] == 128:
                loads[5 + part].wait()
            blocks = [
                dot(fold, raw[part, :, :, 256 * j : 256 * j + 256].reshape(4 * rows, 256))
                for j in range(4)
            ]
            both.append(jnp.concatenate(blocks, axis=1) * taper_ref[...])
        return both

    for t in range(times):
        weight_col = jnp.sum(folds[t], axis=1, keepdims=True)
        if t == 0:
            re, im = fold_sums(folds[0])
        else:
            if t == 1:
                sums[0], sums[1] = fold_sums(jnp.concatenate(folds[1:], axis=0))
            re = sums[0, 128 * t - 128 : 128 * t]
            im = sums[1, 128 * t - 128 : 128 * t]
        xr = [re[:, 256 * j : 256 * j + 256] for j in range(4)]
        xi = [im[:, 256 * j : 256 * j + 256] for j in range(4)]
        if t == 0:
            loads[7].wait()
            loads[8].wait()
        for h in range(4):
            real, imag = spectra(h, xr, xi)
            imag = pltpu.roll(imag.reshape(16, 8, 256), 4, 1).reshape(128, 256)
            scales = []
            for parity in range(2):
                piece = jnp.where(top, real, imag) if parity == 0 else jnp.where(top, imag, real)
                largest = jnp.max(jnp.abs(piece), axis=1, keepdims=True)
                scale = jnp.maximum(largest, 1e-30) * (1.0079 / 32767.0)
                scale = scale.astype(BF16).astype(F32)
                scales.append(scale)
                code = jnp.round(piece * (1.0 / scale)).astype(I32)
                both = jnp.bitwise_or(
                    jnp.left_shift(code[:, 128:], 16), jnp.bitwise_and(code[:, :128], 0xFFFF)
                )
                sent[h, t, parity] = both.reshape(16, 8, 128)
            if h == 0 and t == 0:
                pl.semaphore_wait(barrier, 38)
            if h < 2:
                send_chunk(h, t)
            here = lane == (row % 4) * 64 + 5 + 8 * h + 4 * ((row % 8) // 4) + t
            scale_even = jnp.where(here, scales[0], scale_even)
            scale_odd = jnp.where(here, scales[1], scale_odd)
        if t == 0:
            rank_col = jnp.max(
                jnp.where(slot_row == slot_f, rank_row, 0.0), axis=1, keepdims=True
            )
            by_slot = jnp.where(lane == (row % 4) * 64, rank_col, 0.0)
        by_slot = jnp.where(lane == (row % 4) * 64 + 1 + t, weight_col, by_slot)

    owner32, row32 = iota((32, 128), 0), iota((32, 128), 1)
    meta = (
        dot((row32 // 4 == owner32).astype(F32).astype(BF16), by_slot.astype(BF16))
        + dot((2 * (row32 // 8) == owner32).astype(F32).astype(BF16), scale_even.astype(BF16))
        + dot((2 * (row32 // 8) + 1 == owner32).astype(F32).astype(BF16), scale_odd.astype(BF16))
    )
    for o in range(32):
        meta_out[o] = meta[o : o + 1]
    for i, offset in enumerate(OFFSETS):
        to = partner(offset)
        pltpu.make_async_remote_copy(
            src_ref=meta_out.at[to],
            dst_ref=meta_in.at[i + 1],
            send_sem=meta_send,
            recv_sem=meta_recv,
            device_id=(to, tm),
            device_id_type=MESH,
        ).start()
    for h in range(2, 4):
        for t in range(times):
            send_chunk(h, t)
    meta_in[0] = meta_out[bl]
    for h in range(4):
        for t in range(times):
            held[h, t, 0] = sent[h, t, bl % 2, bl // 2]

    pltpu.make_async_copy(meta_in.at[pl.ds(1, 31)], meta_in.at[pl.ds(1, 31)], meta_recv).wait()
    meta = jnp.concatenate([meta_in[i] for i in range(32)], axis=0)
    held_row, held_lane = iota((256, 128), 0), iota((256, 128), 1)
    expand = (iota((256, 32), 0) // 8 == iota((256, 32), 1)).astype(F32).astype(BF16)
    info = dot(expand, meta.astype(BF16))
    info = jnp.where(held_row % 4 < 2, info[:, :128], info[:, 128:])
    base = (held_row % 2) * 64
    flip = bl % 2

    def column(k):
        return jnp.sum(jnp.where(held_lane == base + k, info, 0.0), axis=1, keepdims=True)

    quadrant = jnp.where(flip == 0, (held_row % 8) // 4, 1 - (held_row % 8) // 4)
    chooser = jnp.where(
        jnp.logical_and(
            column(0) == (held_lane % 64).astype(F32), quadrant == held_lane // 64
        ),
        1.0,
        0.0,
    )
    chooser = jnp.transpose(chooser).astype(BF16)
    weight_mat = jnp.zeros((256, 128), F32)
    for t in range(times):
        weight_mat = jnp.where(held_lane == t, column(1 + t), weight_mat)
    weight_sum = dot(chooser, weight_mat.astype(BF16))
    inverse = 1.0 / jnp.maximum(weight_sum, 1.0)

    def edge(h):
        return pltpu.make_async_remote_copy(
            src_ref=first.at[h],
            dst_ref=after.at[h],
            send_sem=edge_send.at[h],
            recv_sem=edge_recv.at[h],
            device_id=(bl, (tm + 7) % 8),
            device_id_type=MESH,
        )

    for h in range(4):
        power, previous = None, None
        for t in range(times):
            scale_col = column(5 + 8 * h + 4 * ((held_row % 8) // 4) + t)
            pltpu.make_async_copy(
                held.at[h, t, pl.ds(1, 31)], held.at[h, t, pl.ds(1, 31)], recv_sem.at[h, t]
            ).wait()
            both = held[h, t].reshape(256, 128)
            low_part = jnp.right_shift(jnp.left_shift(both, 16), 16)
            high_part = jnp.right_shift(both, 16)
            arrived = jnp.concatenate([low_part, high_part], axis=1).astype(F32) * scale_col
            coarse = arrived.astype(BF16)
            fine = (arrived - coarse.astype(F32)).astype(BF16)
            now = (dot(chooser, coarse) + dot(chooser, fine)) * inverse[:, t : t + 1]
            if t == 0:
                first[h] = now
                edge(h).start()
            elif t == 1:
                power = previous * now
            else:
                power = power + previous * now
            previous = now
        edge(h).wait()
        power = power + jnp.where(tm < 7, previous * after[h], 0.0)
        parts[h] = (power[:64] + power[64:]).reshape(8, 8, 256)
        for e in range(1, 8):
            to = (tm + e) % 8
            pltpu.make_async_remote_copy(
                src_ref=parts.at[h, to],
                dst_ref=fb.at[h, e],
                send_sem=part_send.at[h],
                recv_sem=part_recv.at[h],
                device_id=(bl, to),
                device_id_type=MESH,
            ).start()
        fb[h, 0] = parts[h, tm]

    for h in range(4):
        for t in range(times):
            pltpu.make_async_copy(
                held.at[h, t, pl.ds(1, 31)], held.at[h, t, pl.ds(1, 31)], send_sem.at[h, t]
            ).wait()
    pltpu.make_async_copy(meta_in.at[pl.ds(1, 31)], meta_in.at[pl.ds(1, 31)], meta_send).wait()
    for h in range(4):
        arrivals = fb.at[h, pl.ds(1, 7)]
        pltpu.make_async_copy(arrivals, arrivals, part_send.at[h]).wait()
        pltpu.make_async_copy(arrivals, arrivals, part_recv.at[h]).wait()
        summed = fb[h, 0]
        for e in range(1, 8):
            summed = summed + fb[h, e]
        out_ref[h] = summed


def interleave(x_ref, o_ref):
    lane = iota((8, 128), 1)
    for b in range(8):
        value = jnp.zeros((8, 128), F32)
        for k in range(4):
            source = x_ref[k, :, 128 * (b // 4) : 128 * (b // 4) + 128]
            taken = jnp.take_along_axis(source, 32 * (b % 4) + lane // 4, axis=1)
            value = jnp.where(lane % 4 == k, taken, value)
        o_ref[:, 128 * b : 128 * b + 128] = value


def per_device(visibility_real, visibility_imag, weights, labels, owner_of):
    rows, times, channels = visibility_real.shape
    high, low, twiddle = dft_constants(channels)
    taper = taper_row(channels)
    vmem = pl.BlockSpec(memory_space=pltpu.VMEM)
    hbm = pl.BlockSpec(memory_space=pl.ANY)
    dma = pltpu.SemaphoreType.DMA
    summed = pl.pallas_call(
        kernel,
        out_shape=pltpu.VMEM((4, 8, 256), F32),
        in_specs=[hbm] * 9,
        out_specs=vmem,
        scratch_shapes=[
            pltpu.VMEM((rows,), I32),
            pltpu.VMEM((owner_of.shape[0] // 128, 128), I32),
            pltpu.VMEM((times, rows), I32),
            pltpu.VMEM((1, channels), F32),
            pltpu.VMEM((8, channels // 4), F32),
            pltpu.VMEM((2, rows, times, channels), BF16),
            pltpu.VMEM((2, rows, channels), F32),
            pltpu.VMEM((4, times, 2, 16, 8, 128), I32),
            pltpu.VMEM((4, times, 32, 8, 128), I32),
            pltpu.VMEM((32, 1, 256), F32),
            pltpu.VMEM((32, 1, 256), F32),
            pltpu.VMEM((2, 512, 512), BF16),
            pltpu.VMEM((4, 128, 256), F32),
            pltpu.VMEM((4, 128, 256), F32),
            pltpu.VMEM((4, 8, 8, 256), F32),
            pltpu.VMEM((4, 8, 8, 256), F32),
            dma((9,)),
            dma((4, times)),
            dma((4, times)),
            dma(()),
            dma(()),
            dma((4,)),
            dma((4,)),
            dma((4,)),
            dma((4,)),
        ],
        compiler_params=pltpu.CompilerParams(
            collective_id=0, has_side_effects=True, vmem_limit_bytes=60 * 1024 * 1024
        ),
        name="bandpower",
    )(
        labels, owner_of.reshape(-1, 128), weights.T, jnp.asarray(taper),
        jnp.asarray(twiddle), visibility_real, visibility_imag, jnp.asarray(high), jnp.asarray(low),
    )
    return pl.pallas_call(
        interleave,
        out_shape=jax.ShapeDtypeStruct((8, channels), F32),
        in_specs=[vmem],
        out_specs=vmem,
        name="interleave",
    )(pltpu.with_memory_space_constraint(summed, pltpu.VMEM))


def solution(mesh):
    placed = (P("bl", "tm", None), P("bl", "tm", None), P("bl", "tm"), P("bl"), P())
    return jax.shard_map(
        per_device, mesh=mesh, in_specs=placed, out_specs=P(("bl", "tm"), None), check_vma=False
    )
```

```python
import functools
import math

import jax
import jax.numpy as jnp
import numpy as np
from jax import lax
from jax.experimental import pallas as pl
from jax.experimental.pallas import tpu as pltpu
from jax.sharding import PartitionSpec as P

HARRIS = (0.35875, 0.48829, 0.14128, 0.01168)
MESH = pl.DeviceIdType.MESH
F32, BF16, I32 = jnp.float32, jnp.bfloat16, jnp.int32

OFFSETS = [
    (dz, dx) for dx in (2, 1, 3, 0) for dz in (4, 3, 5, 2, 6, 1, 7, 0) if (dz, dx) != (0, 0)
]


def taper_row(length):
    angle = 2.0 * np.pi / length * np.arange(length)
    h = (
        HARRIS[0]
        - HARRIS[1] * np.cos(angle)
        + HARRIS[2] * np.cos(2.0 * angle)
        - HARRIS[3] * np.cos(3.0 * angle)
    )
    return (h / np.sqrt(np.sum(h * h)))[None, :].astype(np.float32)


def dft_constants(length):
    n = length // 4
    angle = 2.0 * np.pi / n * (np.outer(np.arange(n), np.arange(n)) % n)
    c, s = np.cos(angle), np.sin(angle)
    table = np.block([[c, -s], [s, c]]).astype(np.float32)
    high = table.astype(jnp.bfloat16)
    low = (table - high.astype(np.float32)).astype(jnp.bfloat16)
    turn = 2.0 * np.pi / length * np.outer(np.arange(4), np.arange(n))
    twiddle = np.concatenate([np.cos(turn), np.sin(turn)], axis=0).astype(np.float32)
    return high, low, twiddle


def iota(shape, dim):
    return lax.broadcasted_iota(I32, shape, dim)


def dot(a, b):
    return jnp.dot(a, b, preferred_element_type=F32)


def dot_t(a, b):
    return lax.dot_general(a, b, (((1,), (1,)), ((), ())), preferred_element_type=F32)


def index_rows(labels_ref, owner_ref):
    rows = labels_ref.shape[0]
    blocks = owner_ref.shape[0]
    labels = labels_ref[...].reshape(1, rows)
    high = (labels // 128 == iota((blocks, rows), 0)).astype(F32)
    low = (labels % 128 == iota((128, rows), 0)).astype(F32).astype(BF16)
    present = dot_t(high.astype(BF16), low)
    present = jnp.where(present > 0.0, 1.0, 0.0)
    owner_iota = iota((32, 128), 0)
    hits, marks = [], []
    for b in range(blocks):
        hit = (owner_ref[b : b + 1, :] == owner_iota).astype(F32)
        hits.append(hit)
        marks.append(hit)
        marks.append(hit * present[b : b + 1])
    stacked = jnp.concatenate(marks, axis=0).astype(BF16)
    earlier = jnp.logical_or(iota((128, 256), 0) < iota((128, 256), 1), iota((128, 256), 1) >= 128)
    sums = dot(stacked, earlier.astype(F32).astype(BF16))
    before = jnp.zeros((64, 128), F32)
    ranks, slots = [], []
    for b in range(blocks):
        within = sums[64 * b : 64 * b + 64]
        prefix = within[:, :128] + before
        before = before + within[:, 128:]
        ranks.append(jnp.sum(hits[b] * prefix[:32], axis=0, keepdims=True))
        first_slot = 4.0 * owner_iota.astype(F32)
        slots.append(jnp.sum(hits[b] * (prefix[32:] + first_slot), axis=0, keepdims=True))
    table = jnp.concatenate(slots + ranks, axis=0).astype(BF16)
    found = dot(table, low)
    slot = jnp.sum(high * found[:blocks], axis=0, keepdims=True)
    rank = jnp.sum(high * found[blocks:], axis=0, keepdims=True)
    return slot, rank


def kernel(
    labels_hbm, owner_hbm, weights_hbm, taper_hbm, twiddle_hbm, vis_re, vis_im, high_hbm, low_hbm,
    out_ref,
    labels_ref, owner_ref, weights_ref, taper_ref, twiddle_ref, raw, sums, sent, held,
    meta_out, meta_in, table, first, after, parts, fb,
    load_sem, send_sem, recv_sem, meta_send, meta_recv, edge_send, edge_recv, part_send, part_recv,
):
    bl, tm = lax.axis_index("bl"), lax.axis_index("tm")
    z, x = bl // 4, bl % 4
    times, channels = 4, 1024
    rows = labels_ref.shape[0]

    pairs = [
        (labels_hbm, labels_ref),
        (owner_hbm, owner_ref),
        (weights_hbm, weights_ref),
        (taper_hbm, taper_ref),
        (twiddle_hbm, twiddle_ref),
        (vis_re, raw.at[0]),
        (vis_im, raw.at[1]),
        (high_hbm, table.at[0]),
        (low_hbm, table.at[1]),
    ]
    loads = [
        pltpu.make_async_copy(source, target, load_sem.at[n])
        for n, (source, target) in enumerate(pairs)
    ]
    for load in loads:
        load.start()

    def partner(offset):
        return ((z + offset[0]) % 8) * 4 + (x + offset[1]) % 4

    barrier = pltpu.get_barrier_semaphore()
    for offset in OFFSETS:
        pl.semaphore_signal(barrier, inc=1, device_id=(partner(offset), tm), device_id_type=MESH)
    for e in range(1, 8):
        pl.semaphore_signal(barrier, inc=1, device_id=(bl, (tm + e) % 8), device_id_type=MESH)

    for n in range(5):
        loads[n].wait()
    slot_row, rank_row = index_rows(labels_ref, owner_ref)
    spread = (iota((rows, 4 * rows), 1) // 4 == iota((rows, 4 * rows), 0)).astype(F32).astype(BF16)
    packed = jnp.concatenate(
        [slot_row, weights_ref[...].astype(F32), jnp.zeros((3, rows), F32)], axis=0
    )
    wide = dot(packed.astype(BF16), spread)
    time_of = iota((1, 4 * rows), 1) % 4
    slot_wide = wide[0:1]
    weight_wide = jnp.zeros((1, 4 * rows), F32)
    for t in range(times):
        weight_wide = jnp.where(time_of == t, wide[1 + t : 2 + t], weight_wide)

    slot_f = iota((128, 1), 0).astype(F32)
    lane = iota((128, 128), 1)
    row = iota((128, 128), 0)
    by_slot = None
    scales = jnp.zeros((128, 128), F32)

    cosine = [twiddle_ref[k : k + 1] for k in range(4)]
    sine = [twiddle_ref[4 + k : 5 + k] for k in range(4)]
    top = (iota((128, 1), 0) % 8) < 4

    def send_chunk(h, t):
        for i, offset in enumerate(OFFSETS):
            to = partner(offset)
            pltpu.make_async_remote_copy(
                src_ref=sent.at[h, t, to % 2, to // 2],
                dst_ref=held.at[h, t, i + 1],
                send_sem=send_sem.at[h, t],
                recv_sem=recv_sem.at[h, t],
                device_id=(to, tm),
                device_id_type=MESH,
            ).start()

    def coded(value, inverse_scale):
        code = jnp.round(value * inverse_scale).astype(I32)
        return jnp.bitwise_or(
            jnp.left_shift(code[:, 128:], 16), jnp.bitwise_and(code[:, :128], 0xFFFF)
        )

    def spectra(q, xr, xi):
        if q % 2 == 0:
            ar, ai, br, bi = xr[0] + xr[2], xi[0] + xi[2], xr[1] + xr[3], xi[1] + xi[3]
        else:
            ar, ai, br, bi = xr[0] - xr[2], xi[0] - xi[2], xi[1] - xi[3], xr[3] - xr[1]
        re, im = (ar + br, ai + bi) if q < 2 else (ar - br, ai - bi)
        if q:
            re, im = re * cosine[q] + im * sine[q], im * cosine[q] - re * sine[q]
        y = jnp.concatenate([re, im], axis=1)
        y_high = y.astype(BF16)
        y_low = (y - y_high.astype(F32)).astype(BF16)
        out = dot(y_high, table[0]) + dot(y_low, table[0]) + dot(y_high, table[1])
        return out[:, :256], out[:, 256:]

    folds = [
        jnp.where(jnp.where(time_of == t, slot_wide, -1.0) == slot_f, weight_wide, 0.0)
        for t in range(times)
    ]

    def fold_sums(fold):
        fold = fold.astype(BF16)
        both = []
        for part in range(2):
            if fold.shape[0] == 128:
                loads[5 + part].wait()
            blocks = [
                dot(fold, raw[part, :, :, 256 * j : 256 * j + 256].reshape(4 * rows, 256))
                for j in range(4)
            ]
            both.append(jnp.concatenate(blocks, axis=1) * taper_ref[...])
        return both

    for t in range(times):
        weight_col = jnp.sum(folds[t], axis=1, keepdims=True)
        if t == 0:
            re, im = fold_sums(folds[0])
        else:
            if t == 1:
                sums[0], sums[1] = fold_sums(jnp.concatenate(folds[1:], axis=0))
            re = sums[0, 128 * t - 128 : 128 * t]
            im = sums[1, 128 * t - 128 : 128 * t]
        xr = [re[:, 256 * j : 256 * j + 256] for j in range(4)]
        xi = [im[:, 256 * j : 256 * j + 256] for j in range(4)]
        if t == 0:
            loads[7].wait()
            loads[8].wait()
        for h in range(4):
            real, imag = spectra(h, xr, xi)
            largest = jnp.maximum(
                jnp.max(jnp.abs(real), axis=1, keepdims=True),
                jnp.max(jnp.abs(imag), axis=1, keepdims=True),
            )
            scale = jnp.maximum(largest, 1e-30) * (1.0079 / 32767.0)
            scale = scale.astype(BF16).astype(F32)
            real, imag = coded(real, 1.0 / scale), coded(imag, 1.0 / scale)
            imag = pltpu.roll(imag.reshape(16, 8, 128), 4, 1).reshape(128, 128)
            sent[h, t, 0] = jnp.where(top, real, imag).reshape(16, 8, 128)
            sent[h, t, 1] = jnp.where(top, imag, real).reshape(16, 8, 128)
            if h == 0 and t == 0:
                pl.semaphore_wait(barrier, 38)
            if h < 2:
                send_chunk(h, t)
            scales = jnp.where(lane == (row % 4) * 32 + 5 + 4 * h + t, scale, scales)
        if t == 0:
            rank_col = jnp.max(
                jnp.where(slot_row == slot_f, rank_row, 0.0), axis=1, keepdims=True
            )
            by_slot = jnp.where(lane == (row % 4) * 32, rank_col, 0.0)
        by_slot = jnp.where(lane == (row % 4) * 32 + 1 + t, weight_col, by_slot)

    owner32, row32 = iota((32, 128), 0), iota((32, 128), 1)
    by_slot = (by_slot + scales).astype(BF16)
    meta = dot((row32 // 4 == owner32).astype(F32).astype(BF16), by_slot)
    for o in range(32):
        meta_out[o] = meta[o : o + 1]
    for i, offset in enumerate(OFFSETS):
        to = partner(offset)
        pltpu.make_async_remote_copy(
            src_ref=meta_out.at[to],
            dst_ref=meta_in.at[i + 1],
            send_sem=meta_send,
            recv_sem=meta_recv,
            device_id=(to, tm),
            device_id_type=MESH,
        ).start()
    for h in range(2, 4):
        for t in range(times):
            send_chunk(h, t)
    meta_in[0] = meta_out[bl]
    for h in range(4):
        for t in range(times):
            held[h, t, 0] = sent[h, t, bl % 2, bl // 2]

    pltpu.make_async_copy(meta_in.at[pl.ds(1, 31)], meta_in.at[pl.ds(1, 31)], meta_recv).wait()
    meta = jnp.concatenate([meta_in[i] for i in range(32)], axis=0)
    held_row, held_lane = iota((256, 128), 0), iota((256, 128), 1)
    expand = (iota((256, 32), 0) // 8 == iota((256, 32), 1)).astype(F32).astype(BF16)
    info = dot(expand, meta.astype(BF16))
    base = (held_row % 4) * 32
    flip = bl % 2

    def column(k):
        return jnp.sum(jnp.where(held_lane == base + k, info, 0.0), axis=1, keepdims=True)

    quadrant = jnp.where(flip == 0, (held_row % 8) // 4, 1 - (held_row % 8) // 4)
    chooser = jnp.where(
        jnp.logical_and(
            column(0) == (held_lane % 64).astype(F32), quadrant == held_lane // 64
        ),
        1.0,
        0.0,
    )
    chooser = jnp.transpose(chooser).astype(BF16)
    weight_mat = jnp.zeros((256, 128), F32)
    for t in range(times):
        weight_mat = jnp.where(held_lane == t, column(1 + t), weight_mat)
    weight_sum = dot(chooser, weight_mat.astype(BF16))
    inverse = 1.0 / jnp.maximum(weight_sum, 1.0)

    def edge(h):
        return pltpu.make_async_remote_copy(
            src_ref=first.at[h],
            dst_ref=after.at[h],
            send_sem=edge_send.at[h],
            recv_sem=edge_recv.at[h],
            device_id=(bl, (tm + 7) % 8),
            device_id_type=MESH,
        )

    for h in range(4):
        power, previous = None, None
        for t in range(times):
            scale_col = column(5 + 4 * h + t)
            pltpu.make_async_copy(
                held.at[h, t, pl.ds(1, 31)], held.at[h, t, pl.ds(1, 31)], recv_sem.at[h, t]
            ).wait()
            both = held[h, t].reshape(256, 128)
            low_part = jnp.right_shift(jnp.left_shift(both, 16), 16)
            high_part = jnp.right_shift(both, 16)
            arrived = jnp.concatenate([low_part, high_part], axis=1).astype(F32) * scale_col
            coarse = arrived.astype(BF16)
            fine = (arrived - coarse.astype(F32)).astype(BF16)
            now = (dot(chooser, coarse) + dot(chooser, fine)) * inverse[:, t : t + 1]
            if t == 0:
                first[h] = now
                edge(h).start()
            elif t == 1:
                power = previous * now
            else:
                power = power + previous * now
            previous = now
        edge(h).wait()
        power = power + jnp.where(tm < 7, previous * after[h], 0.0)
        parts[h] = (power[:64] + power[64:]).reshape(8, 8, 256)
        for e in range(1, 8):
            to = (tm + e) % 8
            pltpu.make_async_remote_copy(
                src_ref=parts.at[h, to],
                dst_ref=fb.at[h, e],
                send_sem=part_send.at[h],
                recv_sem=part_recv.at[h],
                device_id=(bl, to),
                device_id_type=MESH,
            ).start()
        fb[h, 0] = parts[h, tm]

    for h in range(4):
        for t in range(times):
            pltpu.make_async_copy(
                held.at[h, t, pl.ds(1, 31)], held.at[h, t, pl.ds(1, 31)], send_sem.at[h, t]
            ).wait()
    pltpu.make_async_copy(meta_in.at[pl.ds(1, 31)], meta_in.at[pl.ds(1, 31)], meta_send).wait()
    for h in range(4):
        arrivals = fb.at[h, pl.ds(1, 7)]
        pltpu.make_async_copy(arrivals, arrivals, part_send.at[h]).wait()
        pltpu.make_async_copy(arrivals, arrivals, part_recv.at[h]).wait()
        summed = fb[h, 0]
        for e in range(1, 8):
            summed = summed + fb[h, e]
        out_ref[h] = summed


def interleave(x_ref, o_ref):
    lane = iota((8, 128), 1)
    for b in range(8):
        value = jnp.zeros((8, 128), F32)
        for k in range(4):
            source = x_ref[k, :, 128 * (b // 4) : 128 * (b // 4) + 128]
            taken = jnp.take_along_axis(source, 32 * (b % 4) + lane // 4, axis=1)
            value = jnp.where(lane % 4 == k, taken, value)
        o_ref[:, 128 * b : 128 * b + 128] = value


def per_device(visibility_real, visibility_imag, weights, labels, owner_of):
    rows, times, channels = visibility_real.shape
    high, low, twiddle = dft_constants(channels)
    taper = taper_row(channels)
    vmem = pl.BlockSpec(memory_space=pltpu.VMEM)
    hbm = pl.BlockSpec(memory_space=pl.ANY)
    dma = pltpu.SemaphoreType.DMA
    summed = pl.pallas_call(
        kernel,
        out_shape=pltpu.VMEM((4, 8, 256), F32),
        in_specs=[hbm] * 9,
        out_specs=vmem,
        scratch_shapes=[
            pltpu.VMEM((rows,), I32),
            pltpu.VMEM((owner_of.shape[0] // 128, 128), I32),
            pltpu.VMEM((times, rows), I32),
            pltpu.VMEM((1, channels), F32),
            pltpu.VMEM((8, channels // 4), F32),
            pltpu.VMEM((2, rows, times, channels), BF16),
            pltpu.VMEM((2, rows, channels), F32),
            pltpu.VMEM((4, times, 2, 16, 8, 128), I32),
            pltpu.VMEM((4, times, 32, 8, 128), I32),
            pltpu.VMEM((32, 1, 128), F32),
            pltpu.VMEM((32, 1, 128), F32),
            pltpu.VMEM((2, 512, 512), BF16),
            pltpu.VMEM((4, 128, 256), F32),
            pltpu.VMEM((4, 128, 256), F32),
            pltpu.VMEM((4, 8, 8, 256), F32),
            pltpu.VMEM((4, 8, 8, 256), F32),
            dma((9,)),
            dma((4, times)),
            dma((4, times)),
            dma(()),
            dma(()),
            dma((4,)),
            dma((4,)),
            dma((4,)),
            dma((4,)),
        ],
        compiler_params=pltpu.CompilerParams(
            collective_id=0, has_side_effects=True, vmem_limit_bytes=60 * 1024 * 1024
        ),
        name="bandpower",
    )(
        labels, owner_of.reshape(-1, 128), weights.T, jnp.asarray(taper),
        jnp.asarray(twiddle), visibility_real, visibility_imag, jnp.asarray(high), jnp.asarray(low),
    )
    return pl.pallas_call(
        interleave,
        out_shape=jax.ShapeDtypeStruct((8, channels), F32),
        in_specs=[vmem],
        out_specs=vmem,
        name="interleave",
    )(pltpu.with_memory_space_constraint(summed, pltpu.VMEM))


def solution(mesh):
    placed = (P("bl", "tm", None), P("bl", "tm", None), P("bl", "tm"), P("bl"), P())
    return jax.shard_map(
        per_device, mesh=mesh, in_specs=placed, out_specs=P(("bl", "tm"), None), check_vma=False
    )
```

```python
import functools
import math

import jax
import jax.numpy as jnp
import numpy as np
from jax import lax
from jax.experimental import pallas as pl
from jax.experimental.pallas import tpu as pltpu
from jax.sharding import PartitionSpec as P

HARRIS = (0.35875, 0.48829, 0.14128, 0.01168)
MESH = pl.DeviceIdType.MESH
F32, BF16, I32 = jnp.float32, jnp.bfloat16, jnp.int32

OFFSETS = [
    (dz, dx) for dx in (2, 1, 3, 0) for dz in (4, 3, 5, 2, 6, 1, 7, 0) if (dz, dx) != (0, 0)
]


def taper_row(length):
    angle = 2.0 * np.pi / length * np.arange(length)
    h = (
        HARRIS[0]
        - HARRIS[1] * np.cos(angle)
        + HARRIS[2] * np.cos(2.0 * angle)
        - HARRIS[3] * np.cos(3.0 * angle)
    )
    return (h / np.sqrt(np.sum(h * h)))[None, :].astype(np.float32)


def dft_constants(length):
    n = length // 4
    angle = 2.0 * np.pi / n * (np.outer(np.arange(n), np.arange(n)) % n)
    c, s = np.cos(angle), np.sin(angle)
    table = np.block([[c, -s], [s, c]]).astype(np.float32)
    high = table.astype(jnp.bfloat16)
    low = (table - high.astype(np.float32)).astype(jnp.bfloat16)
    turn = 2.0 * np.pi / length * np.outer(np.arange(4), np.arange(n))
    twiddle = np.concatenate([np.cos(turn), np.sin(turn)], axis=0).astype(np.float32)
    return high, low, twiddle


def iota(shape, dim):
    return lax.broadcasted_iota(I32, shape, dim)


def dot(a, b):
    return jnp.dot(a, b, preferred_element_type=F32)


def dot_t(a, b):
    return lax.dot_general(a, b, (((1,), (1,)), ((), ())), preferred_element_type=F32)


def index_rows(labels_ref, owner_ref):
    rows = labels_ref.shape[0]
    blocks = owner_ref.shape[0]
    labels = labels_ref[...].reshape(1, rows)
    high = (labels // 128 == iota((blocks, rows), 0)).astype(F32)
    low = (labels % 128 == iota((128, rows), 0)).astype(F32).astype(BF16)
    present = dot_t(high.astype(BF16), low)
    present = jnp.where(present > 0.0, 1.0, 0.0)
    owner_iota = iota((32, 128), 0)
    hits, marks = [], []
    for b in range(blocks):
        hit = (owner_ref[b : b + 1, :] == owner_iota).astype(F32)
        hits.append(hit)
        marks.append(hit)
        marks.append(hit * present[b : b + 1])
    stacked = jnp.concatenate(marks, axis=0).astype(BF16)
    earlier = jnp.logical_or(iota((128, 256), 0) < iota((128, 256), 1), iota((128, 256), 1) >= 128)
    sums = dot(stacked, earlier.astype(F32).astype(BF16))
    before = jnp.zeros((64, 128), F32)
    ranks, slots = [], []
    for b in range(blocks):
        within = sums[64 * b : 64 * b + 64]
        prefix = within[:, :128] + before
        before = before + within[:, 128:]
        ranks.append(jnp.sum(hits[b] * prefix[:32], axis=0, keepdims=True))
        first_slot = 4.0 * owner_iota.astype(F32)
        slots.append(jnp.sum(hits[b] * (prefix[32:] + first_slot), axis=0, keepdims=True))
    table = jnp.concatenate(slots + ranks, axis=0).astype(BF16)
    found = dot(table, low)
    slot = jnp.sum(high * found[:blocks], axis=0, keepdims=True)
    rank = jnp.sum(high * found[blocks:], axis=0, keepdims=True)
    return slot, rank


def kernel(
    labels_hbm, owner_hbm, weights_hbm, taper_hbm, twiddle_hbm, vis_re, vis_im, high_hbm, low_hbm,
    out_ref,
    labels_ref, owner_ref, weights_ref, taper_ref, twiddle_ref, raw, sums, sent, held,
    meta_out, meta_in, table, first, after, parts, fb,
    load_sem, send_sem, recv_sem, meta_send, meta_recv, edge_send, edge_recv, part_send, part_recv,
):
    bl, tm = lax.axis_index("bl"), lax.axis_index("tm")
    z, x = bl // 4, bl % 4
    times, channels = 4, 1024
    rows = labels_ref.shape[0]
    half = rows // 2

    pairs = [
        (labels_hbm, labels_ref),
        (owner_hbm, owner_ref),
        (weights_hbm, weights_ref),
        (taper_hbm, taper_ref),
        (twiddle_hbm, twiddle_ref),
        (vis_re, raw.at[0]),
        (vis_im.at[pl.ds(0, half)], raw.at[1, pl.ds(0, half)]),
        (vis_im.at[pl.ds(half, half)], raw.at[1, pl.ds(half, half)]),
        (high_hbm, table.at[0]),
        (low_hbm, table.at[1]),
    ]
    loads = [
        pltpu.make_async_copy(source, target, load_sem.at[n])
        for n, (source, target) in enumerate(pairs)
    ]
    for load in loads[:8]:
        load.start()

    def partner(offset):
        return ((z + offset[0]) % 8) * 4 + (x + offset[1]) % 4

    barrier = pltpu.get_barrier_semaphore()
    for offset in OFFSETS:
        pl.semaphore_signal(barrier, inc=1, device_id=(partner(offset), tm), device_id_type=MESH)
    for e in range(1, 8):
        pl.semaphore_signal(barrier, inc=1, device_id=(bl, (tm + e) % 8), device_id_type=MESH)

    for n in range(5):
        loads[n].wait()
    slot_row, rank_row = index_rows(labels_ref, owner_ref)
    spread = (iota((rows, 4 * rows), 1) // 4 == iota((rows, 4 * rows), 0)).astype(F32).astype(BF16)
    packed = jnp.concatenate(
        [slot_row, weights_ref[...].astype(F32), jnp.zeros((3, rows), F32)], axis=0
    )
    wide = dot(packed.astype(BF16), spread)
    time_of = iota((1, 4 * rows), 1) % 4
    slot_wide = wide[0:1]
    weight_wide = jnp.zeros((1, 4 * rows), F32)
    for t in range(times):
        weight_wide = jnp.where(time_of == t, wide[1 + t : 2 + t], weight_wide)

    loads[8].start()
    loads[9].start()
    slot_f = iota((128, 1), 0).astype(F32)
    lane = iota((128, 128), 1)
    row = iota((128, 128), 0)
    by_slot = None
    scales = jnp.zeros((128, 128), F32)

    cosine = [twiddle_ref[k : k + 1] for k in range(4)]
    sine = [twiddle_ref[4 + k : 5 + k] for k in range(4)]
    top = (iota((128, 1), 0) % 8) < 4

    def send_chunk(h, t):
        for i, offset in enumerate(OFFSETS):
            to = partner(offset)
            pltpu.make_async_remote_copy(
                src_ref=sent.at[h, t, to % 2, to // 2],
                dst_ref=held.at[h, t, i + 1],
                send_sem=send_sem.at[h, t],
                recv_sem=recv_sem.at[h, t],
                device_id=(to, tm),
                device_id_type=MESH,
            ).start()

    def coded(value, inverse_scale):
        code = jnp.round(value * inverse_scale).astype(I32)
        return jnp.bitwise_or(
            jnp.left_shift(code[:, 128:], 16), jnp.bitwise_and(code[:, :128], 0xFFFF)
        )

    def spectra(q, xr, xi):
        if q % 2 == 0:
            ar, ai, br, bi = xr[0] + xr[2], xi[0] + xi[2], xr[1] + xr[3], xi[1] + xi[3]
        else:
            ar, ai, br, bi = xr[0] - xr[2], xi[0] - xi[2], xi[1] - xi[3], xr[3] - xr[1]
        re, im = (ar + br, ai + bi) if q < 2 else (ar - br, ai - bi)
        if q:
            re, im = re * cosine[q] + im * sine[q], im * cosine[q] - re * sine[q]
        y = jnp.concatenate([re, im], axis=1)
        y_high = y.astype(BF16)
        y_low = (y - y_high.astype(F32)).astype(BF16)
        out = dot(y_high, table[0]) + dot(y_low, table[0]) + dot(y_high, table[1])
        return out[:, :256], out[:, 256:]

    folds = {}

    def fold_of(t):
        if t not in folds:
            slot_t = jnp.where(time_of == t, slot_wide, -1.0)
            folds[t] = jnp.where(slot_t == slot_f, weight_wide, 0.0)
        return folds[t]

    def folded(fold, part, start, count):
        blocks = [
            dot(
                fold[:, 4 * start : 4 * (start + count)],
                raw[part, start : start + count, :, 256 * j : 256 * j + 256].reshape(4 * count, 256),
            )
            for j in range(4)
        ]
        return jnp.concatenate(blocks, axis=1)

    def first_sums(fold):
        fold = fold.astype(BF16)
        loads[5].wait()
        re = folded(fold, 0, 0, rows)
        loads[6].wait()
        im = folded(fold, 1, 0, half)
        loads[7].wait()
        im = im + folded(fold, 1, half, half)
        return re * taper_ref[...], im * taper_ref[...]

    def other_sums(fold):
        fold = fold.astype(BF16)
        return [folded(fold, part, 0, rows) * taper_ref[...] for part in range(2)]

    for t in range(times):
        if t == 0:
            re, im = first_sums(fold_of(0))
        else:
            if t == 1:
                sums[0], sums[1] = other_sums(
                    jnp.concatenate([fold_of(u) for u in range(1, times)], axis=0)
                )
            re = sums[0, 128 * t - 128 : 128 * t]
            im = sums[1, 128 * t - 128 : 128 * t]
        xr = [re[:, 256 * j : 256 * j + 256] for j in range(4)]
        xi = [im[:, 256 * j : 256 * j + 256] for j in range(4)]
        if t == 0:
            loads[8].wait()
            loads[9].wait()
        for h in range(4):
            real, imag = spectra(h, xr, xi)
            largest = jnp.maximum(
                jnp.max(jnp.abs(real), axis=1, keepdims=True),
                jnp.max(jnp.abs(imag), axis=1, keepdims=True),
            )
            scale = jnp.maximum(largest, 1e-30) * (1.0079 / 32767.0)
            scale = scale.astype(BF16).astype(F32)
            real, imag = coded(real, 1.0 / scale), coded(imag, 1.0 / scale)
            imag = pltpu.roll(imag.reshape(16, 8, 128), 4, 1).reshape(128, 128)
            sent[h, t, 0] = jnp.where(top, real, imag).reshape(16, 8, 128)
            sent[h, t, 1] = jnp.where(top, imag, real).reshape(16, 8, 128)
            if h == 0 and t == 0:
                pl.semaphore_wait(barrier, 38)
            if h < 2:
                send_chunk(h, t)
            scales = jnp.where(lane == (row % 4) * 32 + 5 + 4 * h + t, scale, scales)
        if t == 0:
            rank_col = jnp.max(
                jnp.where(slot_row == slot_f, rank_row, 0.0), axis=1, keepdims=True
            )
            by_slot = jnp.where(lane == (row % 4) * 32, rank_col, 0.0)
        weight_col = jnp.sum(fold_of(t), axis=1, keepdims=True)
        by_slot = jnp.where(lane == (row % 4) * 32 + 1 + t, weight_col, by_slot)

    owner32, row32 = iota((32, 128), 0), iota((32, 128), 1)
    by_slot = (by_slot + scales).astype(BF16)
    meta = dot((row32 // 4 == owner32).astype(F32).astype(BF16), by_slot)
    for o in range(32):
        meta_out[o] = meta[o : o + 1]
    for i, offset in enumerate(OFFSETS):
        to = partner(offset)
        pltpu.make_async_remote_copy(
            src_ref=meta_out.at[to],
            dst_ref=meta_in.at[i + 1],
            send_sem=meta_send,
            recv_sem=meta_recv,
            device_id=(to, tm),
            device_id_type=MESH,
        ).start()
    for h in range(2, 4):
        for t in range(times):
            send_chunk(h, t)
    meta_in[0] = meta_out[bl]
    for h in range(4):
        for t in range(times):
            held[h, t, 0] = sent[h, t, bl % 2, bl // 2]

    pltpu.make_async_copy(meta_in.at[pl.ds(1, 31)], meta_in.at[pl.ds(1, 31)], meta_recv).wait()
    meta = jnp.concatenate([meta_in[i] for i in range(32)], axis=0)
    held_row, held_lane = iota((256, 128), 0), iota((256, 128), 1)
    expand = (iota((256, 32), 0) // 8 == iota((256, 32), 1)).astype(F32).astype(BF16)
    info = dot(expand, meta.astype(BF16))
    base = (held_row % 4) * 32
    flip = bl % 2

    def column(k):
        return jnp.sum(jnp.where(held_lane == base + k, info, 0.0), axis=1, keepdims=True)

    quadrant = jnp.where(flip == 0, (held_row % 8) // 4, 1 - (held_row % 8) // 4)
    chooser = jnp.where(
        jnp.logical_and(
            column(0) == (held_lane % 64).astype(F32), quadrant == held_lane // 64
        ),
        1.0,
        0.0,
    )
    chooser = jnp.transpose(chooser).astype(BF16)
    weight_mat = jnp.zeros((256, 128), F32)
    for t in range(times):
        weight_mat = jnp.where(held_lane == t, column(1 + t), weight_mat)
    weight_sum = dot(chooser, weight_mat.astype(BF16))
    inverse = 1.0 / jnp.maximum(weight_sum, 1.0)

    def edge(h):
        return pltpu.make_async_remote_copy(
            src_ref=first.at[h],
            dst_ref=after.at[h],
            send_sem=edge_send.at[h],
            recv_sem=edge_recv.at[h],
            device_id=(bl, (tm + 7) % 8),
            device_id_type=MESH,
        )

    for h in range(4):
        power, previous = None, None
        for t in range(times):
            scale_col = column(5 + 4 * h + t)
            pltpu.make_async_copy(
                held.at[h, t, pl.ds(1, 31)], held.at[h, t, pl.ds(1, 31)], recv_sem.at[h, t]
            ).wait()
            both = held[h, t].reshape(256, 128)
            low_part = jnp.right_shift(jnp.left_shift(both, 16), 16)
            high_part = jnp.right_shift(both, 16)
            arrived = jnp.concatenate([low_part, high_part], axis=1).astype(F32) * scale_col
            coarse = arrived.astype(BF16)
            fine = (arrived - coarse.astype(F32)).astype(BF16)
            now = (dot(chooser, coarse) + dot(chooser, fine)) * inverse[:, t : t + 1]
            if t == 0:
                first[h] = now
                edge(h).start()
            elif t == 1:
                power = previous * now
            else:
                power = power + previous * now
            previous = now
        edge(h).wait()
        power = power + jnp.where(tm < 7, previous * after[h], 0.0)
        parts[h] = (power[:64] + power[64:]).reshape(8, 8, 256)
        for e in (4, 3, 5, 2, 6, 1, 7):
            to = (tm + e) % 8
            pltpu.make_async_remote_copy(
                src_ref=parts.at[h, to],
                dst_ref=fb.at[h, e],
                send_sem=part_send.at[h],
                recv_sem=part_recv.at[h],
                device_id=(bl, to),
                device_id_type=MESH,
            ).start()
        fb[h, 0] = parts[h, tm]

    for h in range(4):
        for t in range(times):
            pltpu.make_async_copy(
                held.at[h, t, pl.ds(1, 31)], held.at[h, t, pl.ds(1, 31)], send_sem.at[h, t]
            ).wait()
    pltpu.make_async_copy(meta_in.at[pl.ds(1, 31)], meta_in.at[pl.ds(1, 31)], meta_send).wait()
    for h in range(4):
        arrivals = fb.at[h, pl.ds(1, 7)]
        pltpu.make_async_copy(arrivals, arrivals, part_send.at[h]).wait()
        pltpu.make_async_copy(arrivals, arrivals, part_recv.at[h]).wait()
        summed = fb[h, 0]
        for e in range(1, 8):
            summed = summed + fb[h, e]
        out_ref[h] = summed


def interleave(x_ref, o_ref):
    lane = iota((8, 128), 1)
    for b in range(8):
        value = jnp.zeros((8, 128), F32)
        for k in range(4):
            source = x_ref[k, :, 128 * (b // 4) : 128 * (b // 4) + 128]
            taken = jnp.take_along_axis(source, 32 * (b % 4) + lane // 4, axis=1)
            value = jnp.where(lane % 4 == k, taken, value)
        o_ref[:, 128 * b : 128 * b + 128] = value


def per_device(visibility_real, visibility_imag, weights, labels, owner_of):
    rows, times, channels = visibility_real.shape
    high, low, twiddle = dft_constants(channels)
    taper = taper_row(channels)
    vmem = pl.BlockSpec(memory_space=pltpu.VMEM)
    hbm = pl.BlockSpec(memory_space=pl.ANY)
    dma = pltpu.SemaphoreType.DMA
    summed = pl.pallas_call(
        kernel,
        out_shape=pltpu.VMEM((4, 8, 256), F32),
        in_specs=[hbm] * 9,
        out_specs=vmem,
        scratch_shapes=[
            pltpu.VMEM((rows,), I32),
            pltpu.VMEM((owner_of.shape[0] // 128, 128), I32),
            pltpu.VMEM((times, rows), I32),
            pltpu.VMEM((1, channels), F32),
            pltpu.VMEM((8, channels // 4), F32),
            pltpu.VMEM((2, rows, times, channels), BF16),
            pltpu.VMEM((2, rows, channels), F32),
            pltpu.VMEM((4, times, 2, 16, 8, 128), I32),
            pltpu.VMEM((4, times, 32, 8, 128), I32),
            pltpu.VMEM((32, 1, 128), F32),
            pltpu.VMEM((32, 1, 128), F32),
            pltpu.VMEM((2, 512, 512), BF16),
            pltpu.VMEM((4, 128, 256), F32),
            pltpu.VMEM((4, 128, 256), F32),
            pltpu.VMEM((4, 8, 8, 256), F32),
            pltpu.VMEM((4, 8, 8, 256), F32),
            dma((10,)),
            dma((4, times)),
            dma((4, times)),
            dma(()),
            dma(()),
            dma((4,)),
            dma((4,)),
            dma((4,)),
            dma((4,)),
        ],
        compiler_params=pltpu.CompilerParams(
            collective_id=0, has_side_effects=True, vmem_limit_bytes=60 * 1024 * 1024
        ),
        name="bandpower",
    )(
        labels, owner_of.reshape(-1, 128), weights.T, jnp.asarray(taper),
        jnp.asarray(twiddle), visibility_real, visibility_imag, jnp.asarray(high), jnp.asarray(low),
    )
    return pl.pallas_call(
        interleave,
        out_shape=jax.ShapeDtypeStruct((8, channels), F32),
        in_specs=[vmem],
        out_specs=vmem,
        name="interleave",
    )(pltpu.with_memory_space_constraint(summed, pltpu.VMEM))


def solution(mesh):
    placed = (P("bl", "tm", None), P("bl", "tm", None), P("bl", "tm"), P("bl"), P())
    return jax.shard_map(
        per_device, mesh=mesh, in_specs=placed, out_specs=P(("bl", "tm"), None), check_vma=False
    )
```
